32 devices in a mesh: cls: 16 (over z, y, x), rep: 2 (over core).
Axes of the slice: x: 2, y: 2, z: 4, core: 2. Of those that a mesh axis runs over, the one named last changes fastest.
Arguments:
- queries: bfloat16 [2, 32, 768], P('rep', 'cls'), may hold values from -16 to 16
- positives: int32 [2, 32, 4], replicated, may hold values from -1 to 98303, as said below
- label_vectors: bfloat16 [98304, 768], P('cls'), may hold values from -80 to 80
- refresh_slot: int32 [], replicated, may hold values from 0 to 7
- features: bfloat16 [12288, 768], P(('cls', 'rep')), may hold values from -6 to 6
- encoder_weight: bfloat16 [768, 768], replicated, may hold values from -0.21875 to 0.21875
- encoder_gain: float32 [768], replicated, may hold values from 0.1 to 1.9
- free_vectors: bfloat16 [12288, 768], P(('cls', 'rep')), may hold values from -3 to 3
- targets: int32 [12288], replicated, may hold values from 0 to 12287, as said below
Outputs:
- loss: float32 [2, 32], P('rep', 'cls')
- query_grads: bfloat16 [2, 32, 768], P('rep', 'cls')
- refreshed_vectors: bfloat16 [12288, 768], P(('cls', 'rep'))
The draws below stay inside these ranges and needn't reach their ends.
Inputs may be any that keep to these rules, and one draw needn't show every extreme that they name: `positives`: each row holds 1 to 4 label ids in its first places and -1 in the rest; ids may repeat within a row. `targets`: A permutation. Refreshed row t belongs to owner t // 768. The b-th aligned block of 384 entries names exactly 24 rows of every owner, all in the half b % 2 of that owner's 768 rows.
All inputs are finite; a program needn't handle non-finite values.
Results may differ from the reference program's by a relative error of at most 0.0048.
Values may be sent and summed in bfloat16 or wider, within the bound.
A program may use at most 128 MiB of HBM per device.

```python
import jax
import jax.numpy as jnp
from jax import lax

D = 768
LAB_DEV = 6144
SLOTS = 8
POS = 4
Q_DEV = 2
LABELS = 98304
R_DEV = 768
REFRESH = 12288
QG = 32
N_CLS = 16
N_REP = 2


def label_rows(key, row_ids):
    row_base = jax.random.fold_in(key, 11)

    def one_row(row_id):
        return jax.random.normal(jax.random.fold_in(row_base, row_id), (D,), jnp.float32)
    values = jnp.clip(jax.vmap(one_row)(row_ids), -6.0, 6.0)
    return values


def draw_label_vectors(key, part):
    return label_rows(key, jnp.arange(LABELS, dtype=jnp.int32)).astype(jnp.bfloat16)


def draw_queries(key, part):
    total_rows = N_REP * Q_DEV * N_CLS
    spread = 3.0 * D ** (-0.5)
    values = spread * jnp.clip(jax.random.normal(jax.random.fold_in(key, 21), (total_rows, D), jnp.float32), -6.0, 6.0)
    return values.reshape(N_REP, Q_DEV * N_CLS, D).astype(jnp.bfloat16)


def draw_positives(key, part):
    total_rows = N_REP * Q_DEV * N_CLS
    counts = jax.random.randint(jax.random.fold_in(key, 31), (total_rows,), 1, POS + 1)
    counts = counts.at[0].set(POS).at[1].set(1)
    label_ids = jax.random.randint(jax.random.fold_in(key, 32), (total_rows, POS), 0, LABELS)
    places = jnp.arange(POS, dtype=jnp.int32)[None, :]
    filled = jnp.where(places < counts[:, None], label_ids, -1)
    return filled.reshape(N_REP, Q_DEV * N_CLS, POS).astype(jnp.int32)


def draw_targets(key, part):
    half_rows = LAB_DEV // SLOTS // N_REP
    per_owner = half_rows // N_CLS
    key_list = jax.random.split(jax.random.fold_in(key, 41), N_REP * N_CLS)
    shuffled = jax.vmap(lambda one_key: jax.random.permutation(one_key, half_rows))(key_list)
    shuffled = shuffled.reshape(N_REP, N_CLS, N_CLS, per_owner)
    owners = jnp.arange(N_CLS, dtype=jnp.int32)[None, :, None, None]
    halves = jnp.arange(N_REP, dtype=jnp.int32)[:, None, None, None]
    rows_all = owners * (half_rows * N_REP) + halves * half_rows + shuffled
    rows_all = rows_all.transpose(2, 0, 1, 3).reshape(N_CLS * N_REP, N_CLS * per_owner)
    order_keys = jax.random.split(jax.random.fold_in(key, 42), N_CLS * N_REP)
    orders = jax.vmap(lambda one_key: jax.random.permutation(one_key, N_CLS * per_owner))(order_keys)
    rows_all = jnp.take_along_axis(rows_all, orders, axis=1)
    return rows_all.reshape(-1).astype(jnp.int32)


def block_levels(key, extent, cuts, low, top_value):
    def one(dim, shards_of):
        heights = jax.random.uniform(jax.random.fold_in(jax.random.fold_in(key, 6), dim), (shards_of,), jnp.float32, low / len(cuts), top_value / len(cuts))
        return jnp.repeat(jnp.exp(heights), extent[dim] // shards_of).reshape((-1,) + (1,) * (len(extent) - dim - 1))

    factor_of = one(*cuts[0])
    for cut in cuts[1:]:
        factor_of = factor_of * one(*cut)
    return factor_of


def normal_values(key, shape, width, limit, cuts=(), held_as=jnp.bfloat16):
    loudness = block_levels(key, shape, cuts, -0.22, 0.18) if cuts else 1.0
    values = jax.random.normal(key, shape, jnp.float32) * width * loudness
    return jnp.minimum(jnp.maximum(values, -limit), limit).astype(held_as)


def setup_inputs(seed: int = 0) -> dict:
    key_of = jax.random.split(jax.random.key(seed), 10)
    return {
        "queries": draw_queries(jax.random.fold_in(key_of[9], 71), 0),
        "positives": draw_positives(jax.random.fold_in(key_of[9], 71), 0),
        "label_vectors": draw_label_vectors(jax.random.fold_in(key_of[9], 71), 0),
        "refresh_slot": jax.random.randint(key_of[3], (), 0, SLOTS).astype(jnp.int32),
        "features": normal_values(key_of[4], (REFRESH, D), 1.0, 6.0, ((0, 32),)),
        "encoder_weight": normal_values(key_of[5], (D, D), D ** -0.5, 0.21875),
        "encoder_gain": jnp.clip(1.0 + 0.18 * jax.random.normal(key_of[6], (D,), jnp.float32), 0.1, 1.9),
        "free_vectors": normal_values(key_of[7], (REFRESH, D), 0.5, 3.0, ((0, 32),)),
        "targets": draw_targets(jax.random.fold_in(key_of[9], 71), 0),
    }


def reference(queries, positives, label_vectors, refresh_slot, features, encoder_weight, encoder_gain, free_vectors, targets):
    hidden = jnp.dot(features, encoder_weight, preferred_element_type=jnp.float32)
    normed = hidden * lax.rsqrt(lax.optimization_barrier(jnp.mean(hidden * hidden, axis=1, keepdims=True)) + 1e-06) * encoder_gain
    encoded = lax.optimization_barrier(normed.astype(jnp.bfloat16))
    placed = jnp.zeros((REFRESH, D), jnp.bfloat16).at[targets].set(encoded)
    refreshed = (free_vectors.astype(jnp.float32) + placed.astype(jnp.float32)).astype(jnp.bfloat16)
    blocks = label_vectors.reshape(N_CLS, SLOTS, R_DEV, D)
    zero_index = jnp.zeros((), jnp.int32)
    current = lax.dynamic_update_slice(blocks, refreshed.reshape(N_CLS, 1, R_DEV, D), (zero_index, refresh_slot.astype(jnp.int32), zero_index, zero_index)).reshape(LABELS, D)
    block_size = Q_DEV * 32
    query_blocks = queries.reshape(-1, block_size, D)
    positive_blocks = positives.reshape(-1, block_size, POS)

    def one_block(block_pair):
        block_queries, block_ids = block_pair
        logits = lax.dot_general(block_queries, current, (((1,), (1,)), ((), ())), preferred_element_type=jnp.float32)
        maximum = lax.optimization_barrier(jnp.max(logits, axis=1))
        exp_total = lax.optimization_barrier(jnp.sum(jnp.exp(logits - maximum[:, None]), axis=1))
        log_total = maximum + jnp.log(exp_total)
        valid_ids = block_ids >= 0
        safe_ids = jnp.where(valid_ids, block_ids, 0).astype(jnp.int32)
        picked = jnp.take_along_axis(logits, safe_ids, axis=1)
        id_count = lax.optimization_barrier(jnp.sum(valid_ids.astype(jnp.float32), axis=1))
        positive_sum = lax.optimization_barrier(jnp.sum(jnp.where(valid_ids, picked, jnp.zeros_like(picked)), axis=1))
        block_loss = log_total - positive_sum / id_count
        id_weight = jnp.where(valid_ids, jnp.ones_like(picked), jnp.zeros_like(picked)) / id_count[:, None]
        row_index = jnp.broadcast_to(jnp.arange(block_ids.shape[0], dtype=jnp.int32)[:, None], block_ids.shape)
        target_mass = jnp.zeros(logits.shape, jnp.float32).at[row_index, safe_ids].add(id_weight)
        coefficients = (jnp.exp(logits - log_total[:, None]) - target_mass).astype(jnp.bfloat16)
        block_grads = jnp.dot(coefficients, current, preferred_element_type=jnp.float32).astype(jnp.bfloat16)
        return (block_loss, block_grads)
    losses, grads = lax.map(one_block, (query_blocks, positive_blocks))
    return (losses.reshape(N_REP, QG), grads.reshape(N_REP, QG, D), refreshed)
```

```python
import functools

import jax
import jax.numpy as jnp
from jax import lax
from jax.experimental import pallas as pl
from jax.experimental.pallas import tpu as pltpu
from jax.sharding import PartitionSpec as P

SLOTS = 8
NEG = -1e30
STATS = 128
NT = (((1,), (1,)), ((), ()))


def to_column(row, eye):
    return jnp.sum(jnp.where(eye, row, 0.0), axis=1, keepdims=True)


def step_kernel(
    n_cls,
    n_rep,
    slot_ref,
    queries_ref,
    positives_ref,
    targets_ref,
    gain_ref,
    labels_hbm,
    features_hbm,
    weight_hbm,
    free_hbm,
    loss_ref,
    grads_ref,
    refreshed_ref,
    labels,
    features,
    weight,
    free,
    q_slots,
    q_rows,
    out_rows,
    in_rows,
    staged,
    logits,
    mixed,
    half_out,
    half_in,
    shares_out,
    shares_in,
    load_sem,
    q_send,
    q_recv,
    row_send,
    row_recv,
    half_send,
    half_recv,
    share_send,
    share_recv,
):
    f32, bf16 = jnp.float32, jnp.bfloat16
    cls = lax.axis_index("cls")
    rep = lax.axis_index("rep")
    total = n_cls * n_rep
    me = cls * n_rep + rep
    half_rows, width = features.shape
    padded = out_rows.shape[1]
    per_owner = half_rows // n_cls
    query_rows = q_slots.shape[1]
    n_query = q_rows.shape[0]
    own_half = n_query // n_rep
    usable, slot_rows = labels.shape[0], half_rows * n_rep
    lab_rows = usable * n_rep

    def slot_of(c, r):
        return r * n_cls + c

    barrier = pltpu.get_barrier_semaphore()

    def greet(k, carry):
        other = lax.rem(me + k, total)
        pl.semaphore_signal(barrier, inc=1, device_id=(other // n_rep, lax.rem(other, n_rep)))
        return carry

    lax.fori_loop(1, total, greet, 0)

    loads = [
        pltpu.make_async_copy(features_hbm, features, load_sem.at[0]),
        pltpu.make_async_copy(weight_hbm, weight, load_sem.at[1]),
        pltpu.make_async_copy(free_hbm, free, load_sem.at[2]),
    ]
    chunks = usable // slot_rows
    for k in range(chunks):
        start = pl.multiple_of(rep * usable + k * slot_rows, slot_rows)
        loads.append(
            pltpu.make_async_copy(
                labels_hbm.at[pl.ds(start, slot_rows)],
                labels.at[pl.ds(k * slot_rows, slot_rows)],
                load_sem.at[3 + k],
            )
        )
    for copy in loads:
        copy.start()

    mine = slot_of(cls, rep)
    q_slots[mine] = queries_ref[0]

    row_i = lax.broadcasted_iota(jnp.int32, (half_rows, half_rows), 0)
    col_i = lax.broadcasted_iota(jnp.int32, (half_rows, half_rows), 1)
    eye = row_i == col_i
    t_row = targets_ref[me].astype(f32)
    t_col = to_column(t_row, eye)
    rank = jnp.sum(jnp.where(t_col < t_row, 1.0, 0.0), axis=0, keepdims=True)
    owner = jnp.floor((rank + 0.5) * (1.0 / per_owner))
    place = owner * padded + (rank - owner * per_owner)
    place_i = lax.broadcasted_iota(jnp.int32, (n_cls * padded, half_rows), 0)
    pick = jnp.where(place_i == place.astype(jnp.int32), 1.0, 0.0).astype(bf16)
    loads[0].wait()
    ordered = jnp.dot(pick, features[...], preferred_element_type=f32).astype(bf16)
    loads[1].wait()
    hidden = jnp.dot(ordered, weight[...], preferred_element_type=f32)
    scale = lax.rsqrt(jnp.mean(hidden * hidden, axis=1, keepdims=True) + 1e-06)
    encoded = hidden * scale * gain_ref[...]
    for c in range(n_cls):
        out_rows[c] = encoded[c * padded : (c + 1) * padded].astype(bf16)

    pl.semaphore_wait(barrier, total - 1)

    def query_copy(other, slot):
        return pltpu.make_async_remote_copy(
            src_ref=q_slots.at[mine],
            dst_ref=q_slots.at[slot],
            send_sem=q_send.at[other],
            recv_sem=q_recv.at[slot],
            device_id=(other // n_rep, lax.rem(other, n_rep)),
        )

    def row_copy(other, slot):
        return pltpu.make_async_remote_copy(
            src_ref=out_rows.at[other],
            dst_ref=in_rows.at[slot],
            send_sem=row_send.at[other],
            recv_sem=row_recv.at[slot],
            device_id=(other, rep),
        )

    def share_copy(other, slot):
        return pltpu.make_async_remote_copy(
            src_ref=shares_out.at[other],
            dst_ref=shares_in.at[slot],
            send_sem=share_send.at[other],
            recv_sem=share_recv.at[slot],
            device_id=(other, rep),
        )

    def send_query(k, carry):
        query_copy(lax.rem(me + k, total), mine).start()
        return carry

    lax.fori_loop(1, total, send_query, 0)

    def send_rows(k, carry):
        row_copy(lax.rem(cls + k, n_cls), cls).start()
        return carry

    lax.fori_loop(1, n_cls, send_rows, 0)
    in_rows[cls] = out_rows[cls]

    my_base = (cls * slot_rows + rep * half_rows).astype(f32)
    wanted = my_base + row_i.astype(f32)

    def find(c, acc):
        t_c = targets_ref[c * n_rep + rep].astype(f32)
        return acc + jnp.where(t_c == wanted, (c + 1).astype(f32), 0.0)

    found = lax.fori_loop(0, n_cls, find, jnp.zeros((half_rows, half_rows), f32))
    src_col = jnp.sum(found, axis=1, keepdims=True) - 1.0
    src_row = jnp.sum(jnp.where(eye, src_col, 0.0), axis=0, keepdims=True)
    before = jnp.where((src_col == src_row) & (col_i < row_i), 1.0, 0.0)
    seat = src_col * padded + jnp.sum(before, axis=1, keepdims=True)
    seat_i = lax.broadcasted_iota(jnp.int32, (half_rows, n_cls * padded), 1)
    seating = jnp.where(seat_i == seat.astype(jnp.int32), 1.0, 0.0).astype(bf16)

    def get_query(k, carry):
        other = lax.rem(me + k, total)
        slot = slot_of(other // n_rep, lax.rem(other, n_rep))
        query_copy(other, slot).wait_recv()
        return carry

    lax.fori_loop(1, total, get_query, 0)
    for s in range(total):
        q_rows[s * query_rows : (s + 1) * query_rows] = q_slots[s].astype(f32)
    q = q_rows[...].astype(bf16)

    ids = positives_ref[...]
    slot_start = slot_ref[0] * slot_rows
    n_pos = ids.shape[1]

    def counts_of(first, cols):
        label = first + lax.broadcasted_iota(jnp.int32, (n_query, cols), 1)
        count = jnp.zeros((n_query, cols), f32)
        for p in range(n_pos):
            count = count + jnp.where(ids[:, p : p + 1] == label, 1.0, 0.0)
        return count

    def weighted(block, peak, count, vectors):
        power = jnp.exp(block - peak)
        high = power.astype(bf16)
        low = (power - high.astype(f32)).astype(bf16)
        n = n_query
        cols = block.shape[1]
        mixed[0:n, 0:cols] = high
        mixed[n : 2 * n, 0:cols] = low
        mixed[2 * n : 3 * n, 0:cols] = count.astype(bf16)
        out = jnp.dot(mixed[:, 0:cols], vectors, preferred_element_type=f32)
        exp_sum = jnp.sum(power, axis=1, keepdims=True)
        pos_sum = jnp.sum(count * jnp.where(count > 0.0, block, 0.0), axis=1, keepdims=True)
        return out[0:n] + out[n : 2 * n], out[2 * n : 3 * n], exp_sum, pos_sum

    peak = jnp.full((n_query, 1), NEG, f32)
    for k in range(chunks):
        loads[3 + k].wait()
        at = slice(k * slot_rows, (k + 1) * slot_rows)
        block = lax.dot_general(q, labels[at], NT, preferred_element_type=f32)
        fresh = slot_start == rep * usable + k * slot_rows
        block = jnp.where(fresh, NEG, block)
        logits[:, at] = block
        peak = jnp.maximum(peak, jnp.max(block, axis=1, keepdims=True))
    grad = jnp.zeros((n_query, width), f32)
    hits = jnp.zeros((n_query, width), f32)
    exp_sum = jnp.zeros((n_query, 1), f32)
    pos_sum = jnp.zeros((n_query, 1), f32)
    for k in range(chunks):
        at = slice(k * slot_rows, (k + 1) * slot_rows)
        first = cls * lab_rows + rep * usable + k * slot_rows
        fresh = slot_start == rep * usable + k * slot_rows
        count = jnp.where(fresh, 0.0, counts_of(first, slot_rows))
        g, t, e, s = weighted(logits[:, at], peak, count, labels[at])
        grad, hits, exp_sum, pos_sum = grad + g, hits + t, exp_sum + e, pos_sum + s

    fresh_count = counts_of(cls * lab_rows + slot_start + rep * half_rows, half_rows)

    def get_rows(k, carry):
        other = lax.rem(cls + n_cls - k, n_cls)
        row_copy(other, other).wait_recv()
        return carry

    lax.fori_loop(1, n_cls, get_rows, 0)
    for c in range(n_cls):
        staged[c * padded : (c + 1) * padded] = in_rows[c].astype(f32)
    placed = jnp.dot(seating, staged[...].astype(bf16), preferred_element_type=f32)
    loads[2].wait()
    refreshed_ref[...] = (free[...].astype(f32) + placed).astype(bf16)
    vectors = refreshed_ref[...]
    block = lax.dot_general(q, vectors, NT, preferred_element_type=f32)
    fresh_peak = jnp.max(block, axis=1, keepdims=True)
    g, t, e, s = weighted(block, fresh_peak, fresh_count, vectors)
    top = jnp.maximum(peak, fresh_peak)
    a, b = jnp.exp(peak - top), jnp.exp(fresh_peak - top)
    grad, hits = grad * a + g * b, hits + t
    exp_sum, pos_sum = exp_sum * a + e * b, pos_sum + s

    lane = lax.broadcasted_iota(jnp.int32, (n_query, STATS), 1)
    stats = jnp.where(lane == 0, top, jnp.where(lane == 1, exp_sum, pos_sum))
    for r in range(n_rep):
        at = slice(r * own_half, (r + 1) * own_half)
        half_out[r, :, 0:width] = grad[at]
        half_out[r, :, width : 2 * width] = hits[at]
        half_out[r, :, 2 * width :] = stats[at]
    partner = 1 - rep
    swap = pltpu.make_async_remote_copy(
        src_ref=half_out.at[partner],
        dst_ref=half_in,
        send_sem=half_send,
        recv_sem=half_recv,
        device_id=(cls, partner),
    )
    swap.start()

    def merge(x, y):
        xs, ys = x[:, 2 * width :], y[:, 2 * width :]
        m = jnp.maximum(xs[:, 0:1], ys[:, 0:1])
        a, b = jnp.exp(xs[:, 0:1] - m), jnp.exp(ys[:, 0:1] - m)
        both = x[:, 0:width] * a + y[:, 0:width] * b
        return (
            both,
            x[:, width : 2 * width] + y[:, width : 2 * width],
            m,
            xs[:, 1:2] * a + ys[:, 1:2] * b,
            xs[:, 2:3] + ys[:, 2:3],
        )

    swap.wait_recv()
    both, hits, m, exp_sum, pos_sum = merge(half_out[rep], half_in[...])
    lane = lax.broadcasted_iota(jnp.int32, (own_half, STATS), 1)
    stats = jnp.where(lane == 0, m, jnp.where(lane == 1, exp_sum, pos_sum))
    for c in range(n_cls):
        at = slice(c * query_rows, (c + 1) * query_rows)
        shares_out[c, :, 0:width] = both[at]
        shares_out[c, :, width : 2 * width] = hits[at]
        shares_out[c, :, 2 * width :] = stats[at]

    def send_share(k, carry):
        share_copy(lax.rem(cls + k, n_cls), cls).start()
        return carry

    lax.fori_loop(1, n_cls, send_share, 0)
    shares_in[cls] = shares_out[cls]

    own_ids = positives_ref[pl.ds(mine * query_rows, query_rows), :]
    id_count = jnp.sum(jnp.where(own_ids >= 0, 1.0, 0.0), axis=1, keepdims=True)

    def get_share(k, carry):
        other = lax.rem(cls + n_cls - k, n_cls)
        share_copy(other, other).wait_recv()
        return carry

    lax.fori_loop(1, n_cls, get_share, 0)

    def peak_of(c, m):
        return jnp.maximum(m, shares_in[c, :, 2 * width : 2 * width + 1])

    m = lax.fori_loop(0, n_cls, peak_of, jnp.full((query_rows, 1), NEG, f32))

    def add(c, state):
        grad, hits, exp_sum, pos_sum = state
        share = shares_in[c]
        a = jnp.exp(share[:, 2 * width : 2 * width + 1] - m)
        return (
            grad + a * share[:, 0:width],
            hits + share[:, width : 2 * width],
            exp_sum + a * share[:, 2 * width + 1 : 2 * width + 2],
            pos_sum + share[:, 2 * width + 2 : 2 * width + 3],
        )

    zero = jnp.zeros((query_rows, 1), f32)
    wide = jnp.zeros((query_rows, width), f32)
    grad, hits, exp_sum, pos_sum = lax.fori_loop(0, n_cls, add, (wide, wide, zero, zero))
    loss = m + jnp.log(exp_sum) - pos_sum / id_count
    loss_ref[...] = jnp.broadcast_to(loss, loss_ref.shape)
    grads_ref[0] = (grad / exp_sum - hits / id_count).astype(bf16)

    def end_query(k, carry):
        query_copy(lax.rem(me + k, total), mine).wait_send()
        return carry

    lax.fori_loop(1, total, end_query, 0)

    def end_rows(k, carry):
        other = lax.rem(cls + k, n_cls)
        row_copy(other, cls).wait_send()
        share_copy(other, cls).wait_send()
        return carry

    lax.fori_loop(1, n_cls, end_rows, 0)
    swap.wait_send()


def per_device(
    n_cls,
    n_rep,
    queries,
    positives,
    label_vectors,
    refresh_slot,
    features,
    encoder_weight,
    encoder_gain,
    free_vectors,
    targets,
):
    f32, bf16 = jnp.float32, jnp.bfloat16
    total = n_cls * n_rep
    lab_rows, width = label_vectors.shape
    usable = lab_rows // n_rep
    slot_rows = lab_rows // SLOTS
    half_rows = slot_rows // n_rep
    per_owner = half_rows // n_cls
    padded = -(-per_owner // 8) * 8
    query_rows = queries.shape[1]
    n_query = total * query_rows
    share = 2 * width + STATS
    vmem = pl.BlockSpec(memory_space=pltpu.VMEM)
    smem = pl.BlockSpec(memory_space=pltpu.SMEM)
    hbm = pl.BlockSpec(memory_space=pl.ANY)
    dma = pltpu.SemaphoreType.DMA
    loss, grads, refreshed = pl.pallas_call(
        functools.partial(step_kernel, n_cls, n_rep),
        out_shape=(
            jax.ShapeDtypeStruct((query_rows, 128), f32),
            jax.ShapeDtypeStruct((1, query_rows, width), bf16),
            jax.ShapeDtypeStruct((half_rows, width), bf16),
        ),
        in_specs=[smem, vmem, vmem, vmem, vmem, hbm, hbm, hbm, hbm],
        out_specs=(vmem, vmem, vmem),
        scratch_shapes=[
            pltpu.VMEM((usable, width), bf16),
            pltpu.VMEM((half_rows, width), bf16),
            pltpu.VMEM((width, width), bf16),
            pltpu.VMEM((half_rows, width), bf16),
            pltpu.VMEM((total, query_rows, width), bf16),
            pltpu.VMEM((n_query, width), f32),
            pltpu.VMEM((n_cls, padded, width), bf16),
            pltpu.VMEM((n_cls, padded, width), bf16),
            pltpu.VMEM((n_cls * padded, width), f32),
            pltpu.VMEM((n_query, usable), f32),
            pltpu.VMEM((3 * n_query, slot_rows), bf16),
            pltpu.VMEM((n_rep, n_query // n_rep, share), f32),
            pltpu.VMEM((n_query // n_rep, share), f32),
            pltpu.VMEM((n_cls, query_rows, share), f32),
            pltpu.VMEM((n_cls, query_rows, share), f32),
            dma((3 + usable // slot_rows,)),
            dma((total,)),
            dma((total,)),
            dma((n_cls,)),
            dma((n_cls,)),
            dma,
            dma,
            dma((n_cls,)),
            dma((n_cls,)),
        ],
        compiler_params=pltpu.CompilerParams(
            collective_id=0, has_side_effects=True, vmem_limit_bytes=60 * 2**20
        ),
    )(
        refresh_slot.reshape(1),
        queries,
        positives.reshape(n_query, positives.shape[2]),
        targets.reshape(total, 1, half_rows),
        encoder_gain.reshape(1, width),
        label_vectors,
        features,
        encoder_weight,
        free_vectors,
    )
    return loss[:, 0].reshape(1, query_rows), grads, refreshed


def solution(mesh):
    placed = (
        P("rep", "cls", None),
        P(),
        P("cls", None),
        P(),
        P(("cls", "rep"), None),
        P(),
        P(),
        P(("cls", "rep"), None),
        P(),
    )
    return jax.shard_map(
        functools.partial(per_device, mesh.shape["cls"], mesh.shape["rep"]),
        mesh=mesh,
        in_specs=placed,
        out_specs=(P("rep", "cls"), P("rep", "cls", None), P(("cls", "rep"), None)),
        check_vma=False,
    )
```

```python
import functools

import jax
import jax.numpy as jnp
from jax import lax
from jax.experimental import pallas as pl
from jax.experimental.pallas import tpu as pltpu
from jax.sharding import PartitionSpec as P

SLOTS = 8
NEG = -1e30
STATS = 128
NT = (((1,), (1,)), ((), ()))


def to_column(row, eye):
    return jnp.sum(jnp.where(eye, row, 0.0), axis=1, keepdims=True)


def eye_of(n):
    shape = (n, n)
    return lax.broadcasted_iota(jnp.int32, shape, 0) == lax.broadcasted_iota(jnp.int32, shape, 1)


def step_kernel(
    n_cls,
    n_rep,
    slot_ref,
    queries_ref,
    positives_ref,
    targets_ref,
    gain_ref,
    labels_hbm,
    features_hbm,
    weight_hbm,
    free_hbm,
    loss_ref,
    grads_ref,
    refreshed_hbm,
    labels,
    features,
    weight,
    free,
    fresh_rows,
    id_counts,
    q_slots,
    q_rows,
    out_rows,
    in_rows,
    staged,
    logits,
    mixed,
    half_out,
    half_in,
    shares_out,
    shares_in,
    load_sem,
    q_send,
    q_recv,
    relay_send,
    relay_recv,
    fresh_sem,
    row_send,
    row_recv,
    half_send,
    half_recv,
    share_send,
    share_recv,
):
    f32, bf16 = jnp.float32, jnp.bfloat16
    cls = lax.axis_index("cls")
    rep = lax.axis_index("rep")
    total = n_cls * n_rep
    me = cls * n_rep + rep
    half_rows, width = features.shape
    padded = out_rows.shape[1]
    per_owner = half_rows // n_cls
    query_rows = q_slots.shape[1]
    n_query = q_rows.shape[0]
    own_half = n_query // n_rep
    usable, slot_rows = labels.shape[0], half_rows * n_rep
    lab_rows = usable * n_rep

    def slot_of(c, r):
        return r * n_cls + c

    barrier = pltpu.get_barrier_semaphore()

    def greet(k, carry):
        other = lax.rem(me + k, total)
        pl.semaphore_signal(barrier, inc=1, device_id=(other // n_rep, lax.rem(other, n_rep)))
        return carry

    lax.fori_loop(1, total, greet, 0)

    loads = [
        pltpu.make_async_copy(features_hbm, features, load_sem.at[0]),
        pltpu.make_async_copy(weight_hbm, weight, load_sem.at[1]),
        pltpu.make_async_copy(free_hbm, free, load_sem.at[2]),
    ]
    chunks = usable // slot_rows
    for k in range(chunks):
        start = pl.multiple_of(rep * usable + k * slot_rows, slot_rows)
        loads.append(
            pltpu.make_async_copy(
                labels_hbm.at[pl.ds(start, slot_rows)],
                labels.at[pl.ds(k * slot_rows, slot_rows)],
                load_sem.at[3 + k],
            )
        )
    for copy in loads:
        copy.start()

    mine = slot_of(cls, rep)
    q_slots[mine] = queries_ref[0]

    row_i = lax.broadcasted_iota(jnp.int32, (half_rows, half_rows), 0)
    col_i = lax.broadcasted_iota(jnp.int32, (half_rows, half_rows), 1)
    eye = row_i == col_i
    t_row = targets_ref[me].astype(f32)
    t_col = to_column(t_row, eye)
    rank = jnp.sum(jnp.where(t_col < t_row, 1.0, 0.0), axis=0, keepdims=True)
    owner = jnp.floor((rank + 0.5) * (1.0 / per_owner))
    place = owner * padded + (rank - owner * per_owner)
    place_i = lax.broadcasted_iota(jnp.int32, (n_cls * padded, half_rows), 0)
    pick = jnp.where(place_i == place.astype(jnp.int32), 1.0, 0.0).astype(bf16)
    loads[0].wait()
    ordered = jnp.dot(pick, features[...], preferred_element_type=f32).astype(bf16)
    loads[1].wait()
    hidden = jnp.dot(ordered, weight[...], preferred_element_type=f32)
    scale = lax.rsqrt(jnp.mean(hidden * hidden, axis=1, keepdims=True) + 1e-06)
    encoded = hidden * scale * gain_ref[...].reshape(1, width)
    for c in range(n_cls):
        out_rows[c] = encoded[c * padded : (c + 1) * padded].astype(bf16)

    pl.semaphore_wait(barrier, total - 1)

    partner = 1 - rep

    def far(k):
        return lax.rem(cls + 1 + lax.rem(k + n_cls // 2 - 2, n_cls - 1), n_cls)

    def far_from(k):
        return lax.rem(cls + n_cls - 1 - lax.rem(k + n_cls // 2 - 2, n_cls - 1), n_cls)

    def query_copy(other, slot):
        return pltpu.make_async_remote_copy(
            src_ref=q_slots.at[mine],
            dst_ref=q_slots.at[slot],
            send_sem=q_send.at[other],
            recv_sem=q_recv.at[slot],
            device_id=(other, rep),
        )

    def row_copy(other, slot):
        return pltpu.make_async_remote_copy(
            src_ref=out_rows.at[other],
            dst_ref=in_rows.at[slot],
            send_sem=row_send.at[other],
            recv_sem=row_recv.at[slot],
            device_id=(other, rep),
        )

    def share_copy(other, slot):
        return pltpu.make_async_remote_copy(
            src_ref=shares_out.at[other],
            dst_ref=shares_in.at[slot],
            send_sem=share_send.at[other],
            recv_sem=share_recv.at[slot],
            device_id=(other, rep),
        )

    def send_query(k, carry):
        query_copy(far(k), mine).start()
        return carry

    lax.fori_loop(1, n_cls, send_query, 0)

    def send_rows(k, carry):
        row_copy(far(k), cls).start()
        return carry

    lax.fori_loop(1, n_cls, send_rows, 0)
    in_rows[cls] = out_rows[cls]

    def get_query(k, carry):
        other = far_from(k)
        query_copy(other, slot_of(other, rep)).wait_recv()
        return carry

    lax.fori_loop(1, n_cls, get_query, 0)
    side = q_slots.at[pl.ds(rep * n_cls, n_cls)]
    relay = pltpu.make_async_remote_copy(
        src_ref=side,
        dst_ref=side,
        send_sem=relay_send,
        recv_sem=relay_recv,
        device_id=(cls, partner),
    )
    relay.start()

    my_base = (cls * slot_rows + rep * half_rows).astype(f32)
    wanted = my_base + row_i.astype(f32)

    def find(c, acc):
        t_c = targets_ref[c * n_rep + rep].astype(f32)
        return acc + jnp.where(t_c == wanted, (c + 1).astype(f32), 0.0)

    found = lax.fori_loop(0, n_cls, find, jnp.zeros((half_rows, half_rows), f32))
    src_col = jnp.sum(found, axis=1, keepdims=True) - 1.0
    src_row = jnp.sum(jnp.where(eye, src_col, 0.0), axis=0, keepdims=True)
    before = jnp.where((src_col == src_row) & (col_i < row_i), 1.0, 0.0)
    seat = src_col * padded + jnp.sum(before, axis=1, keepdims=True)
    seat_i = lax.broadcasted_iota(jnp.int32, (half_rows, n_cls * padded), 1)
    seating = jnp.where(seat_i == seat.astype(jnp.int32), 1.0, 0.0).astype(bf16)

    relay.wait_recv()
    for s in range(total):
        q_rows[s * query_rows : (s + 1) * query_rows] = q_slots[s].astype(f32)
    q = q_rows[...].astype(bf16)

    n_pos = positives_ref.shape[1]
    eye = eye_of(own_half)
    ids = []
    for p in range(n_pos):
        rows = [positives_ref[r, p : p + 1, :].astype(f32) for r in range(n_rep)]
        ids.append(jnp.concatenate([to_column(row, eye) for row in rows], axis=0).astype(jnp.int32))
    valid = jnp.zeros((n_query, 1), f32)
    for p in range(n_pos):
        valid = valid + jnp.where(ids[p] >= 0, 1.0, 0.0)
    id_counts[...] = jnp.broadcast_to(valid, id_counts.shape)
    slot_start = slot_ref[0] * slot_rows

    def counts_of(first, cols):
        label = first + lax.broadcasted_iota(jnp.int32, (n_query, cols), 1)
        count = jnp.zeros((n_query, cols), f32)
        for p in range(n_pos):
            count = count + jnp.where(ids[p] == label, 1.0, 0.0)
        return count

    def weighted(block, peak, count, vectors):
        power = jnp.exp(block - peak)
        high = power.astype(bf16)
        low = (power - high.astype(f32)).astype(bf16)
        n = n_query
        cols = block.shape[1]
        mixed[0:n, 0:cols] = high
        mixed[n : 2 * n, 0:cols] = low
        mixed[2 * n : 3 * n, 0:cols] = count.astype(bf16)
        out = jnp.dot(mixed[:, 0:cols], vectors, preferred_element_type=f32)
        exp_sum = jnp.sum(power, axis=1, keepdims=True)
        pos_sum = jnp.sum(count * jnp.where(count > 0.0, block, 0.0), axis=1, keepdims=True)
        return out[0:n] + out[n : 2 * n], out[2 * n : 3 * n], exp_sum, pos_sum

    peak = jnp.full((n_query, 1), NEG, f32)
    for k in range(chunks):
        loads[3 + k].wait()
        at = slice(k * slot_rows, (k + 1) * slot_rows)
        block = lax.dot_general(q, labels[at], NT, preferred_element_type=f32)
        fresh = slot_start == rep * usable + k * slot_rows
        block = jnp.where(fresh, NEG, block)
        logits[:, at] = block
        peak = jnp.maximum(peak, jnp.max(block, axis=1, keepdims=True))
    grad = jnp.zeros((n_query, width), f32)
    hits = jnp.zeros((n_query, width), f32)
    exp_sum = jnp.zeros((n_query, 1), f32)
    pos_sum = jnp.zeros((n_query, 1), f32)
    for k in range(chunks):
        at = slice(k * slot_rows, (k + 1) * slot_rows)
        first = cls * lab_rows + rep * usable + k * slot_rows
        fresh = slot_start == rep * usable + k * slot_rows
        count = jnp.where(fresh, 0.0, counts_of(first, slot_rows))
        g, t, e, s = weighted(logits[:, at], peak, count, labels[at])
        grad, hits, exp_sum, pos_sum = grad + g, hits + t, exp_sum + e, pos_sum + s

    fresh_count = counts_of(cls * lab_rows + slot_start + rep * half_rows, half_rows)

    def stage(c):
        staged[pl.ds(pl.multiple_of(c * padded, 8), padded)] = in_rows[c].astype(f32)

    def get_rows(k, carry):
        other = far_from(k)
        row_copy(other, other).wait_recv()
        stage(other)
        return carry

    stage(cls)
    lax.fori_loop(1, n_cls, get_rows, 0)
    placed = jnp.dot(seating, staged[...].astype(bf16), preferred_element_type=f32)
    loads[2].wait()
    fresh_rows[...] = (free[...].astype(f32) + placed).astype(bf16)
    vectors = fresh_rows[...]
    store = pltpu.make_async_copy(fresh_rows, refreshed_hbm, fresh_sem)
    store.start()
    block = lax.dot_general(q, vectors, NT, preferred_element_type=f32)
    fresh_peak = jnp.max(block, axis=1, keepdims=True)
    g, t, e, s = weighted(block, fresh_peak, fresh_count, vectors)
    top = jnp.maximum(peak, fresh_peak)
    a, b = jnp.exp(peak - top), jnp.exp(fresh_peak - top)
    grad, hits = grad * a + g * b, hits + t
    exp_sum, pos_sum = exp_sum * a + e * b, pos_sum + s

    lane = lax.broadcasted_iota(jnp.int32, (n_query, STATS), 1)
    stats = jnp.where(lane == 0, top, jnp.where(lane == 1, exp_sum, pos_sum))
    for r in range(n_rep):
        at = slice(r * own_half, (r + 1) * own_half)
        half_out[r, :, 0:width] = grad[at]
        half_out[r, :, width : 2 * width] = hits[at]
        half_out[r, :, 2 * width :] = stats[at]
    swap = pltpu.make_async_remote_copy(
        src_ref=half_out.at[partner],
        dst_ref=half_in,
        send_sem=half_send,
        recv_sem=half_recv,
        device_id=(cls, partner),
    )
    swap.start()

    def merge(x, y):
        xs, ys = x[:, 2 * width :], y[:, 2 * width :]
        m = jnp.maximum(xs[:, 0:1], ys[:, 0:1])
        a, b = jnp.exp(xs[:, 0:1] - m), jnp.exp(ys[:, 0:1] - m)
        both = x[:, 0:width] * a + y[:, 0:width] * b
        return (
            both,
            x[:, width : 2 * width] + y[:, width : 2 * width],
            m,
            xs[:, 1:2] * a + ys[:, 1:2] * b,
            xs[:, 2:3] + ys[:, 2:3],
        )

    swap.wait_recv()
    both, hits, m, exp_sum, pos_sum = merge(half_out[rep], half_in[...])
    lane = lax.broadcasted_iota(jnp.int32, (own_half, STATS), 1)
    stats = jnp.where(lane == 0, m, jnp.where(lane == 1, exp_sum, pos_sum))
    for c in range(n_cls):
        at = slice(c * query_rows, (c + 1) * query_rows)
        shares_out[c, :, 0:width] = both[at]
        shares_out[c, :, width : 2 * width] = hits[at]
        shares_out[c, :, 2 * width :] = stats[at]

    def send_share(k, carry):
        share_copy(far(k), cls).start()
        return carry

    lax.fori_loop(1, n_cls, send_share, 0)
    shares_in[cls] = shares_out[cls]

    id_count = id_counts[pl.ds(mine * query_rows, query_rows), :][:, 0:1]

    def get_share(k, carry):
        other = far_from(k)
        share_copy(other, other).wait_recv()
        return carry

    lax.fori_loop(1, n_cls, get_share, 0)

    def peak_of(c, m):
        return jnp.maximum(m, shares_in[c, :, 2 * width : 2 * width + 1])

    m = lax.fori_loop(0, n_cls, peak_of, jnp.full((query_rows, 1), NEG, f32))

    def add(c, state):
        grad, hits, exp_sum, pos_sum = state
        share = shares_in[c]
        a = jnp.exp(share[:, 2 * width : 2 * width + 1] - m)
        return (
            grad + a * share[:, 0:width],
            hits + share[:, width : 2 * width],
            exp_sum + a * share[:, 2 * width + 1 : 2 * width + 2],
            pos_sum + share[:, 2 * width + 2 : 2 * width + 3],
        )

    zero = jnp.zeros((query_rows, 1), f32)
    wide = jnp.zeros((query_rows, width), f32)
    grad, hits, exp_sum, pos_sum = lax.fori_loop(0, n_cls, add, (wide, wide, zero, zero))
    loss = m + jnp.log(exp_sum) - pos_sum / id_count
    loss_ref[...] = jnp.sum(jnp.where(eye_of(query_rows), loss, 0.0), axis=0, keepdims=True)
    grads_ref[0] = (grad / exp_sum - hits / id_count).astype(bf16)

    def end_rows(k, carry):
        other = lax.rem(cls + k, n_cls)
        query_copy(other, mine).wait_send()
        row_copy(other, cls).wait_send()
        share_copy(other, cls).wait_send()
        return carry

    lax.fori_loop(1, n_cls, end_rows, 0)
    swap.wait_send()
    relay.wait_send()
    store.wait()


def pass_on(*refs):
    half = len(refs) // 2
    for source, target in zip(refs[:half], refs[half:]):
        target[...] = source[...]


def per_device(
    n_cls,
    n_rep,
    queries,
    positives,
    label_vectors,
    refresh_slot,
    features,
    encoder_weight,
    encoder_gain,
    free_vectors,
    targets,
):
    f32, bf16 = jnp.float32, jnp.bfloat16
    total = n_cls * n_rep
    lab_rows, width = label_vectors.shape
    usable = lab_rows // n_rep
    slot_rows = lab_rows // SLOTS
    half_rows = slot_rows // n_rep
    per_owner = half_rows // n_cls
    padded = -(-per_owner // 8) * 8
    query_rows = queries.shape[1]
    n_query = total * query_rows
    share = 2 * width + STATS
    vmem = pl.BlockSpec(memory_space=pltpu.VMEM)
    smem = pl.BlockSpec(memory_space=pltpu.SMEM)
    hbm = pl.BlockSpec(memory_space=pl.ANY)
    dma = pltpu.SemaphoreType.DMA
    outs = (
        jax.ShapeDtypeStruct((1, query_rows), f32),
        jax.ShapeDtypeStruct((1, query_rows, width), bf16),
        jax.ShapeDtypeStruct((half_rows, width), bf16),
    )
    results = pl.pallas_call(
        functools.partial(step_kernel, n_cls, n_rep),
        out_shape=outs,
        in_specs=[smem, vmem, vmem, vmem, vmem, hbm, hbm, hbm, hbm],
        out_specs=(vmem, vmem, hbm),
        scratch_shapes=[
            pltpu.VMEM((usable, width), bf16),
            pltpu.VMEM((half_rows, width), bf16),
            pltpu.VMEM((width, width), bf16),
            pltpu.VMEM((half_rows, width), bf16),
            pltpu.VMEM((half_rows, width), bf16),
            pltpu.VMEM((n_query, STATS), f32),
            pltpu.VMEM((total, query_rows, width), bf16),
            pltpu.VMEM((n_query, width), f32),
            pltpu.VMEM((n_cls, padded, width), bf16),
            pltpu.VMEM((n_cls, padded, width), bf16),
            pltpu.VMEM((n_cls * padded, width), f32),
            pltpu.VMEM((n_query, usable), f32),
            pltpu.VMEM((3 * n_query, slot_rows), bf16),
            pltpu.VMEM((n_rep, n_query // n_rep, share), f32),
            pltpu.VMEM((n_query // n_rep, share), f32),
            pltpu.VMEM((n_cls, query_rows, share), f32),
            pltpu.VMEM((n_cls, query_rows, share), f32),
            dma((3 + usable // slot_rows,)),
            dma((n_cls,)),
            dma((total,)),
            dma,
            dma,
            dma,
            dma((n_cls,)),
            dma((n_cls,)),
            dma,
            dma,
            dma((n_cls,)),
            dma((n_cls,)),
        ],
        compiler_params=pltpu.CompilerParams(
            collective_id=0, has_side_effects=True, vmem_limit_bytes=60 * 2**20
        ),
    )(
        refresh_slot.reshape(1),
        queries,
        positives.transpose(0, 2, 1),
        targets.reshape(total, 1, half_rows),
        encoder_gain,
        label_vectors,
        features,
        encoder_weight,
        free_vectors,
    )
    return pl.pallas_call(
        pass_on,
        out_shape=outs,
        in_specs=[vmem] * 3,
        out_specs=(vmem,) * 3,
    )(*results)


def solution(mesh):
    placed = (
        P("rep", "cls", None),
        P(),
        P("cls", None),
        P(),
        P(("cls", "rep"), None),
        P(),
        P(),
        P(("cls", "rep"), None),
        P(),
    )
    return jax.shard_map(
        functools.partial(per_device, mesh.shape["cls"], mesh.shape["rep"]),
        mesh=mesh,
        in_specs=placed,
        out_specs=(P("rep", "cls"), P("rep", "cls", None), P(("cls", "rep"), None)),
        check_vma=False,
    )
```
